32 devices in a mesh: dom: 16 (over z, x, core), rep: 2 (over y).
Axes of the slice: x: 2, y: 2, z: 4, core: 2. Of those that a mesh axis runs over, the one named last changes fastest.
Arguments:
- node_feats: bfloat16 [12288, 256], P(('dom', 'rep')), may hold values from -6 to 6
- node_ids: int32 [12288], replicated, may hold values from 0 to 16777215
- tile_row: int32 [16, 2, 16], replicated, may hold values from -1 to 95, as said below
- tile_col: int32 [16, 2, 16], replicated, may hold values from -1 to 95, as said below
- tile_count: int32 [16, 2, 16], replicated, may hold values from 1 to 128, as said below
- self_weight: bfloat16 [256, 512], replicated, may hold values from -0.375 to 0.375
- neigh_weight: bfloat16 [256, 512], replicated, may hold values from -3 to 3
- out_grad: bfloat16 [12288, 512], P(('dom', 'rep')), may hold values from -6 to 6
Outputs:
- hidden_out: bfloat16 [12288, 512], P(('dom', 'rep'))
- feat_grad: bfloat16 [12288, 256], P(('dom', 'rep'))
- self_grad: float32 [256, 512], replicated
- neigh_grad: float32 [256, 512], replicated
The draws below stay inside these ranges and needn't reach their ends.
Inputs may be any that keep to these rules, and one draw needn't show every extreme that they name: `tile_row`: entry [d, r, s] is -1 where the slot holds no tile, else a block row of dom group d: d * 6 plus 0 to 5. In every draw some pair (d, r) has all 16 of its slots filled. `tile_col`: -1 exactly where tile_row is -1; else one of the blocks of device (s, r): s * 6 + r * 3 plus 0 to 2. `tile_count`: read only where a tile is present.
All inputs are finite; a program needn't handle non-finite values.
Results may differ from the reference program's by a relative error of at most 0.01.
Values may be sent and summed in bfloat16 or wider, within the bound.
A program may use at most 64 MiB of HBM per device.

```python
import math
import jax
import jax.numpy as jnp
from jax import lax

TILE = 128
F_IN = 256
F_OUT = 512
BPD = 3
NODES = 12288
N_DOM = 16
N_REP = 2


def tile_pattern(key):
    folded = jax.random.fold_in(key, 4242)
    subkeys = jax.random.split(folded, 9)
    slot_shape = (N_DOM, N_REP, N_DOM)
    group_blocks = BPD * N_REP
    fill_rates = jax.random.randint(subkeys[0], (N_DOM, 1, 1), 2, 9)
    filled = jax.random.randint(subkeys[1], slot_shape, 0, 8) < fill_rates
    full_dom = jax.random.randint(subkeys[2], (), 0, N_DOM)
    full_rep = jax.random.randint(subkeys[3], (), 0, N_REP)
    forced = (jnp.arange(N_DOM)[:, None, None] == full_dom) & (jnp.arange(N_REP)[None, :, None] == full_rep)
    filled = filled | forced
    first_draw = jax.random.randint(subkeys[4], slot_shape, 0, group_blocks)
    second = jax.random.randint(subkeys[5], slot_shape, 0, group_blocks)
    row_order = jax.random.permutation(subkeys[6], group_blocks)
    local_row = row_order[jnp.minimum(first_draw, second)]
    row_block = jnp.arange(N_DOM)[:, None, None] * group_blocks + local_row
    col_block = jnp.arange(N_DOM)[None, None, :] * group_blocks + jnp.arange(N_REP)[None, :, None] * BPD + jax.random.randint(subkeys[7], slot_shape, 0, BPD)
    count_draws = jax.random.randint(subkeys[8], (2,) + slot_shape, 1, TILE + 1)
    counts = (count_draws[0] * count_draws[1] + TILE - 1) // TILE
    return (jnp.where(filled, row_block, -1).astype(jnp.int32), jnp.where(filled, col_block, -1).astype(jnp.int32), counts.astype(jnp.int32))


def draw_tile_row(key, part):
    return tile_pattern(key)[0]


def draw_tile_col(key, part):
    return tile_pattern(key)[1]


def draw_tile_count(key, part):
    return tile_pattern(key)[2]


def set_ends(result, key, low, top_value):
    extent = result.shape
    place = [jax.random.randint(jax.random.fold_in(key, axis), (), 0, extent[axis]) for axis in range(len(extent))]
    result = result.at[tuple(place)].set(low)
    longest = extent.index(max(extent))
    place[longest] = (place[longest] + 1) % extent[longest]
    return result.at[tuple(place)].set(top_value)


def levels(rng, extent, shards, least, top_value):
    factor_of, own = 1.0, jax.random.fold_in(rng, 6)
    for axis_at, blocks in shards:
        draws = jnp.exp(jax.random.uniform(jax.random.fold_in(own, axis_at), (blocks,), jnp.float32, least / len(shards), top_value / len(shards)))
        factor_of = factor_of * jnp.repeat(draws, extent[axis_at] // blocks).reshape([-1 if axis == axis_at else 1 for axis in range(len(extent))])
    return factor_of


def centred(own_key, extent, deviation, limit, cuts=(), kind=jnp.bfloat16):
    result = jax.random.normal(own_key, extent, jnp.float32) * deviation
    if len(cuts) > 0:
        result = levels(own_key, extent, cuts, -0.22, 0.18) * result
    return jnp.clip(result, min=-limit, max=limit).astype(kind)


def setup_inputs(seed: int = 0) -> dict:
    keys = jax.random.split(jax.random.key(seed), 9)
    return {
        "node_feats": centred(keys[0], (NODES, F_IN), 1.0, 6.0, ((0, 32),)),
        "node_ids": set_ends(jax.random.randint(keys[1], (NODES,), 0, 16777216 // ((NODES + 65520) // 65521)), jax.random.fold_in(keys[1], 1), 0, (16777216 // ((NODES + 65520) // 65521)) - 1).astype(jnp.int32),
        "tile_row": draw_tile_row(jax.random.fold_in(keys[8], 71), 0),
        "tile_col": draw_tile_col(jax.random.fold_in(keys[8], 71), 0),
        "tile_count": draw_tile_count(jax.random.fold_in(keys[8], 71), 0),
        "self_weight": centred(keys[5], (F_IN, F_OUT), F_IN ** -0.5, 0.375),
        "neigh_weight": centred(keys[6], (F_IN, F_OUT), (max(F_IN // 64, 1)) ** -0.5, 3.0),
        "out_grad": centred(keys[7], (NODES, F_OUT), 1.0, 6.0, ((0, 32),)),
    }


def edge_masks(row_ids, col_ids, limits):
    left_ids = (row_ids % 4093)[:, :, None]
    right_ids = (col_ids % 4091)[:, None, :]
    hashed = (left_ids * right_ids + left_ids + 3 * right_ids) % 4099 % TILE
    return (hashed < limits[:, None, None]).astype(jnp.float32)

def slot_masks(id_blocks, rows_in, cols_in, limits_in):
    present = rows_in >= 0
    row_block = jnp.where(present, rows_in, 0)
    col_block = jnp.where(present, cols_in, 0)
    limits = jnp.where(present, limits_in, 0)
    tile_masks = edge_masks(id_blocks[row_block], id_blocks[col_block], limits)
    return (tile_masks, row_block, col_block, present)

def reference(node_feats, node_ids, tile_row, tile_col, tile_count, self_weight, neigh_weight, out_grad):
    node_count, width_in = node_feats.shape
    block_count = node_count // TILE
    group_blocks = block_count // N_DOM
    id_blocks = node_ids.reshape(block_count, TILE)
    feat_blocks = node_feats.astype(jnp.float32).reshape(block_count, TILE, width_in)

    def forward_group(group_index):
        tile_masks, row_block, col_block, present = slot_masks(id_blocks, tile_row[group_index].reshape(-1), tile_col[group_index].reshape(-1), tile_count[group_index].reshape(-1))
        products = jnp.einsum('sij,sjf->sif', tile_masks, feat_blocks[col_block])
        offset = row_block - group_index * group_blocks
        select = ((offset[:, None] == jnp.arange(group_blocks)[None, :]) & present[:, None]).astype(jnp.float32)
        partial_value = jnp.einsum('rsb,rsif->rbif', select.reshape(N_REP, N_DOM, group_blocks), products.reshape(N_REP, N_DOM, TILE, width_in))
        rounded = lax.optimization_barrier(partial_value.astype(jnp.bfloat16))
        return lax.optimization_barrier(jnp.sum(rounded.astype(jnp.float32), axis=0))
    summed = lax.map(forward_group, jnp.arange(N_DOM)).reshape(node_count, width_in)
    flat_rows = tile_row.reshape(-1)
    flat_limits = tile_count.reshape(-1)
    present_all = flat_rows >= 0
    degree = jnp.zeros((block_count,), jnp.float32).at[jnp.where(present_all, flat_rows, 0)].add(jnp.where(present_all, flat_limits, 0).astype(jnp.float32))
    divisor = jnp.repeat(jnp.maximum(degree, 1.0), TILE)[:, None]
    mean_feats = (summed / divisor).astype(jnp.bfloat16)
    preact = jnp.dot(node_feats, self_weight, preferred_element_type=jnp.float32) + jnp.dot(mean_feats, neigh_weight, preferred_element_type=jnp.float32)
    hidden_out = jax.nn.silu(preact).astype(jnp.bfloat16)
    logistic = jax.nn.sigmoid(preact)
    pre_grad = (out_grad.astype(jnp.float32) * logistic * (1.0 + preact * (1.0 - logistic))).astype(jnp.bfloat16)
    grad_scale = 1.0 / math.sqrt(node_count)
    self_grad = jnp.dot(node_feats.T, pre_grad, preferred_element_type=jnp.float32) * grad_scale
    neigh_grad = jnp.dot(mean_feats.T, pre_grad, preferred_element_type=jnp.float32) * grad_scale
    mean_grad = jnp.dot(pre_grad, neigh_weight.T, preferred_element_type=jnp.float32)
    spread = (mean_grad / divisor).astype(jnp.bfloat16)
    spread_blocks = spread.astype(jnp.float32).reshape(block_count, TILE, width_in)

    def backward_group(running, group_index):
        tile_masks, row_block, col_block, present = slot_masks(id_blocks, tile_row[group_index].reshape(-1), tile_col[group_index].reshape(-1), tile_count[group_index].reshape(-1))
        products = jnp.einsum('sij,sif->sjf', tile_masks, spread_blocks[row_block])
        return (running.at[col_block].add(products), None)
    transposed, _ = lax.scan(backward_group, jnp.zeros((block_count, TILE, width_in), jnp.float32), jnp.arange(N_DOM))
    feat_grad = (jnp.dot(pre_grad, self_weight.T, preferred_element_type=jnp.float32) + transposed.reshape(node_count, width_in)).astype(jnp.bfloat16)
    return (hidden_out, feat_grad, self_grad, neigh_grad)
```

```python
import math

import jax
import jax.numpy as jnp
from jax import lax
from jax.sharding import PartitionSpec as P

TILE = 128


def edge_masks(row_ids, col_ids, limits, tile_size):
    left_ids = (row_ids % 4093)[:, :, None]
    right_ids = (col_ids % 4091)[:, None, :]
    hashed = (left_ids * right_ids + left_ids + 3 * right_ids) % 4099 % tile_size
    return (hashed < limits[:, None, None]).astype(jnp.bfloat16)


def shards(
    node_feats, node_ids, tile_row, tile_col, tile_count, self_weight, neigh_weight, out_grad
):
    dom_total = lax.axis_size("dom")
    rep_total = lax.axis_size("rep")
    dom_here = lax.axis_index("dom")
    rep_here = lax.axis_index("rep")
    rows_here, width_in = node_feats.shape
    blocks_here = rows_here // TILE
    group_blocks = blocks_here * rep_total
    id_blocks = node_ids.reshape(-1, TILE)
    group_first = dom_here * group_blocks
    own_first = group_first + rep_here * blocks_here
    inbound_rows = tile_row[dom_here, rep_here]
    inbound_present = inbound_rows >= 0
    inbound_block = jnp.where(inbound_present, inbound_rows, 0)
    inbound_cols = jnp.where(inbound_present, tile_col[dom_here, rep_here], 0)
    inbound_limits = jnp.where(inbound_present, tile_count[dom_here, rep_here], 0)
    inbound_masks = edge_masks(
        id_blocks[inbound_block], id_blocks[inbound_cols], inbound_limits, TILE
    )
    inbound_offset = jnp.where(inbound_present, inbound_block - group_first, 0)
    row_select = (
        (jnp.arange(group_blocks)[:, None] == inbound_offset[None, :]) & inbound_present[None, :]
    ).astype(jnp.float32)
    outbound_cols = tile_col[:, rep_here, dom_here]
    outbound_present = outbound_cols >= 0
    outbound_offset = jnp.where(outbound_present, outbound_cols - own_first, 0)
    own_select = (
        (outbound_offset[:, None] == jnp.arange(blocks_here)[None, :]) & outbound_present[:, None]
    ).astype(jnp.float32)
    feat_blocks = node_feats.reshape(blocks_here, TILE, width_in)
    outgoing = feat_blocks[outbound_offset]
    products = jnp.einsum(
        "sij,sjf->sif",
        inbound_masks,
        lax.all_to_all(outgoing, "dom", split_axis=0, concat_axis=0, tiled=True),
        preferred_element_type=jnp.float32,
    )
    partial_value = jnp.einsum("bs,sif->bif", row_select, products)
    partial_parts = lax.all_to_all(
        partial_value.reshape(rep_total, rows_here, width_in).astype(jnp.bfloat16),
        "rep",
        split_axis=0,
        concat_axis=0,
        tiled=True,
    )
    summed = jnp.sum(partial_parts.astype(jnp.float32), axis=0)
    group_rows = tile_row[dom_here].reshape(-1)
    group_limits = tile_count[dom_here].reshape(-1)
    owned_rows = group_rows[:, None] == own_first + jnp.arange(blocks_here)[None, :]
    degree = jnp.sum(jnp.where(owned_rows, group_limits[:, None], 0), axis=0).astype(jnp.float32)
    divisor = jnp.repeat(jnp.maximum(degree, 1.0), TILE)[:, None]
    mean_feats = (summed / divisor).astype(jnp.bfloat16)
    preact = jnp.dot(node_feats, self_weight, preferred_element_type=jnp.float32) + jnp.dot(
        mean_feats, neigh_weight, preferred_element_type=jnp.float32
    )
    hidden_out = jax.nn.silu(preact).astype(jnp.bfloat16)
    logistic = jax.nn.sigmoid(preact)
    pre_grad = (out_grad.astype(jnp.float32) * logistic * (1.0 + preact * (1.0 - logistic))).astype(
        jnp.bfloat16
    )
    over_rows = (((0,), (0,)), ((), ()))
    over_cols = (((1,), (1,)), ((), ()))
    self_term = lax.dot_general(node_feats, pre_grad, over_rows, preferred_element_type=jnp.float32)
    neigh_term = lax.dot_general(
        mean_feats, pre_grad, over_rows, preferred_element_type=jnp.float32
    )
    grad_scale = 1.0 / math.sqrt(rows_here * dom_total * rep_total)
    both_terms = jnp.concatenate([self_term, neigh_term], axis=0).astype(jnp.bfloat16)
    both_rows, width_out = both_terms.shape
    devices = dom_total * rep_total
    both_parts = lax.all_to_all(
        both_terms.reshape(devices, both_rows // devices, width_out),
        ("dom", "rep"),
        split_axis=0,
        concat_axis=0,
        tiled=True,
    )
    both_share = jnp.sum(both_parts.astype(jnp.float32), axis=0) * grad_scale
    both_grads = lax.all_gather(
        both_share.astype(jnp.bfloat16), ("dom", "rep"), axis=0, tiled=True
    ).astype(jnp.float32)
    mean_grad = lax.dot_general(
        pre_grad, neigh_weight, over_cols, preferred_element_type=jnp.float32
    )
    spread = (mean_grad / divisor).astype(jnp.bfloat16)
    group_spread = lax.all_gather(spread, "rep", axis=0, tiled=True).reshape(
        group_blocks, TILE, width_in
    )
    picked_rows = group_spread[inbound_offset]
    products = jnp.einsum(
        "sij,sif->sjf", inbound_masks, picked_rows, preferred_element_type=jnp.float32
    )
    returned = lax.all_to_all(
        products.astype(jnp.bfloat16), "dom", split_axis=0, concat_axis=0, tiled=True
    ).astype(products.dtype)
    transposed = jnp.einsum("db,djf->bjf", own_select, returned)
    self_back = lax.dot_general(
        pre_grad, self_weight, over_cols, preferred_element_type=jnp.float32
    )
    feat_grad = (self_back + transposed.reshape(rows_here, width_in)).astype(jnp.bfloat16)
    return (hidden_out, feat_grad, both_grads[: both_rows // 2], both_grads[both_rows // 2 :])


def solution(mesh):
    placed = (P(("dom", "rep"), None), P(), P(), P(), P(), P(), P(), P(("dom", "rep"), None))
    return jax.shard_map(
        shards,
        mesh=mesh,
        in_specs=placed,
        out_specs=(P(("dom", "rep"), None), P(("dom", "rep"), None), P(), P()),
        check_vma=False,
    )
```

```python
import functools
import math

import jax
import jax.numpy as jnp
from jax import lax
from jax.experimental import pallas as pl
from jax.experimental.pallas import tpu as pltpu
from jax.sharding import PartitionSpec as P

TILE = 128

MESH = pl.DeviceIdType.MESH
OVER_ROWS = (((0,), (0,)), ((), ()))
OVER_COLS = (((1,), (1,)), ((), ()))


def greet(devices):
    barrier = pltpu.get_barrier_semaphore()
    for device in devices:
        pl.semaphore_signal(barrier, inc=1, device_id=device, device_id_type=MESH)
    pl.semaphore_wait(barrier, len(devices))


def send(src, dst, sems, slot, device):
    copy = pltpu.make_async_remote_copy(
        src_ref=src,
        dst_ref=dst,
        send_sem=sems.at[0, slot],
        recv_sem=sems.at[1, slot],
        device_id=device,
        device_id_type=MESH,
    )
    copy.start()
    return copy


def dom_exchange(dom_total, src, dst, sems):
    me, rep = lax.axis_index("dom"), lax.axis_index("rep")
    peers = [lax.rem(me + k, dom_total) for k in range(1, dom_total)]
    greet([(peer, rep) for peer in peers])
    copies = [
        send(src.at[peer], dst.at[me], sems, k, (peer, rep)) for k, peer in enumerate(peers)
    ]
    dst[me] = src[me]
    for copy in copies:
        copy.wait()


def dense(
    rep_total, partials, divisor, feats, w_self, w_neigh, cotangent,
    hidden, terms, back, gathered, landed, mine, sems_in, sems_out,
):
    dom, me = lax.axis_index("dom"), lax.axis_index("rep")
    peers = [lax.rem(me + k, rep_total) for k in range(1, rep_total)]
    greet([(dom, peer) for peer in peers])
    copies = [
        send(partials.at[peer], landed.at[k], sems_in, k, (dom, peer))
        for k, peer in enumerate(peers)
    ]
    x = feats[...]
    preact = jnp.dot(x, w_self[...], preferred_element_type=jnp.float32)
    summed = partials[me].astype(jnp.float32)
    for k, copy in enumerate(copies):
        copy.wait()
        summed = summed + landed[k].astype(jnp.float32)
    div = divisor[...]
    mean = (summed / div).astype(jnp.bfloat16)
    preact = preact + jnp.dot(mean, w_neigh[...], preferred_element_type=jnp.float32)
    logistic = jax.nn.sigmoid(preact)
    grad = (
        cotangent[...].astype(jnp.float32) * logistic * (1.0 + preact * (1.0 - logistic))
    ).astype(jnp.bfloat16)
    spread = lax.dot_general(grad, w_neigh[...], OVER_COLS, preferred_element_type=jnp.float32)
    mine[...] = (spread / div).astype(jnp.bfloat16)
    copies = [
        send(mine, gathered.at[me], sems_out, k, (dom, peer)) for k, peer in enumerate(peers)
    ]
    gathered[me] = mine[...]
    hidden[...] = (preact * logistic).astype(jnp.bfloat16)
    terms[0] = lax.dot_general(
        x, grad, OVER_ROWS, preferred_element_type=jnp.float32
    ).astype(jnp.bfloat16)
    terms[1] = lax.dot_general(
        mean, grad, OVER_ROWS, preferred_element_type=jnp.float32
    ).astype(jnp.bfloat16)
    back[...] = lax.dot_general(grad, w_self[...], OVER_COLS, preferred_element_type=jnp.float32)
    for copy in copies:
        copy.wait()


def finish(
    dom_total, rep_total, inner, scale, terms, products, grads, returned,
    landed, share, strips, final, sems_a, sems_b, sems_c, sems_d, sems_e,
):
    dom, rep = lax.axis_index("dom"), lax.axis_index("rep")
    outer = dom_total // inner
    plane = inner * rep_total
    layer, within = dom // inner, lax.rem(dom, inner)
    spot = within * rep_total + rep
    plane_peers = []
    for k in range(1, plane):
        other = lax.rem(spot + k, plane)
        plane_peers.append(
            (other, (layer * inner + other // rep_total, lax.rem(other, rep_total)))
        )
    layer_peers = []
    for k in range(1, outer):
        other = lax.rem(layer + k, outer)
        layer_peers.append((other, (other * inner + within, rep)))
    dom_peers = [lax.rem(dom + k, dom_total) for k in range(1, dom_total)]
    greet([device for _, device in plane_peers] + [(peer, rep) for peer in dom_peers])
    first = [
        send(terms.at[other], landed.at[k], sems_a, k, device)
        for k, (other, device) in enumerate(plane_peers)
    ]
    exchange = [
        send(products.at[peer], returned.at[dom], sems_e, k, (peer, rep))
        for k, peer in enumerate(dom_peers)
    ]
    returned[dom] = products[dom]
    total = terms[spot].astype(jnp.float32)
    for k, copy in enumerate(first):
        copy.wait()
        total = total + landed[k].astype(jnp.float32)
    share[...] = total.astype(jnp.bfloat16)
    second = [
        send(share.at[other], strips.at[k], sems_b, k, device)
        for k, (other, device) in enumerate(layer_peers)
    ]
    total = share[layer].astype(jnp.float32)
    for k, copy in enumerate(second):
        copy.wait()
        total = total + strips[k].astype(jnp.float32)
    final[...] = (total * scale).astype(jnp.bfloat16)
    third = [
        send(final, grads.at[spot, layer], sems_c, k, device)
        for k, (_, device) in enumerate(layer_peers)
    ]
    grads[spot, layer] = final[...]
    for copy in third:
        copy.wait()
    fourth = [
        send(grads.at[spot], grads.at[spot], sems_d, k, device)
        for k, (_, device) in enumerate(plane_peers)
    ]
    for copy in fourth + exchange:
        copy.wait()


def pair_sems(count):
    return pltpu.SemaphoreType.DMA((2, max(count, 1)))


def call(kernel, out_shapes, scratch, ident, *operands):
    return pl.pallas_call(
        kernel,
        out_shape=out_shapes,
        in_specs=[pl.BlockSpec(memory_space=pltpu.VMEM)] * len(operands),
        out_specs=jax.tree.map(lambda _: pl.BlockSpec(memory_space=pltpu.VMEM), out_shapes),
        scratch_shapes=scratch,
        compiler_params=pltpu.CompilerParams(collective_id=ident, has_side_effects=True),
    )(*operands)


def edge_masks(row_ids, col_ids, limits, tile_size):
    left_ids = (row_ids % 4093)[:, :, None]
    right_ids = (col_ids % 4091)[:, None, :]
    hashed = (left_ids * right_ids + left_ids + 3 * right_ids) % 4099 % tile_size
    return (hashed < limits[:, None, None]).astype(jnp.bfloat16)


def shards(
    node_feats, node_ids, tile_row, tile_col, tile_count, self_weight, neigh_weight, out_grad
):
    dom_total = lax.axis_size("dom")
    rep_total = lax.axis_size("rep")
    dom_here = lax.axis_index("dom")
    rep_here = lax.axis_index("rep")
    rows_here, width_in = node_feats.shape
    blocks_here = rows_here // TILE
    group_blocks = blocks_here * rep_total
    id_blocks = node_ids.reshape(-1, TILE)
    group_first = dom_here * group_blocks
    own_first = group_first + rep_here * blocks_here
    inbound_rows = tile_row[dom_here, rep_here]
    inbound_present = inbound_rows >= 0
    inbound_block = jnp.where(inbound_present, inbound_rows, 0)
    inbound_cols = jnp.where(inbound_present, tile_col[dom_here, rep_here], 0)
    inbound_limits = jnp.where(inbound_present, tile_count[dom_here, rep_here], 0)
    inbound_masks = edge_masks(
        id_blocks[inbound_block], id_blocks[inbound_cols], inbound_limits, TILE
    )
    inbound_offset = jnp.where(inbound_present, inbound_block - group_first, 0)
    row_select = (
        (jnp.arange(group_blocks)[:, None] == inbound_offset[None, :]) & inbound_present[None, :]
    ).astype(jnp.float32)
    outbound_cols = tile_col[:, rep_here, dom_here]
    outbound_present = outbound_cols >= 0
    outbound_offset = jnp.where(outbound_present, outbound_cols - own_first, 0)
    own_select = (
        (outbound_offset[:, None] == jnp.arange(blocks_here)[None, :]) & outbound_present[:, None]
    ).astype(jnp.float32)
    feat_blocks = node_feats.reshape(blocks_here, TILE, width_in)
    outgoing = feat_blocks[outbound_offset]
    products = jnp.einsum(
        "sij,sjf->sif",
        inbound_masks,
        call(
            functools.partial(dom_exchange, dom_total),
            jax.ShapeDtypeStruct(outgoing.shape, jnp.bfloat16),
            [pair_sems(dom_total - 1)],
            0,
            outgoing,
        ),
        preferred_element_type=jnp.float32,
    )
    partial_value = jnp.einsum("bs,sif->bif", row_select, products)
    group_rows = tile_row[dom_here].reshape(-1)
    group_limits = tile_count[dom_here].reshape(-1)
    owned_rows = group_rows[:, None] == own_first + jnp.arange(blocks_here)[None, :]
    degree = jnp.sum(jnp.where(owned_rows, group_limits[:, None], 0), axis=0).astype(jnp.float32)
    divisor = jnp.repeat(jnp.maximum(degree, 1.0), TILE)[:, None]
    width_out = self_weight.shape[1]
    hidden_out, both_terms, self_back, group_spread = call(
        functools.partial(dense, rep_total),
        (
            jax.ShapeDtypeStruct((rows_here, width_out), jnp.bfloat16),
            jax.ShapeDtypeStruct((2, width_in, width_out), jnp.bfloat16),
            jax.ShapeDtypeStruct((rows_here, width_in), jnp.float32),
            jax.ShapeDtypeStruct((rep_total, rows_here, width_in), jnp.bfloat16),
        ),
        [
            pltpu.VMEM((max(rep_total - 1, 1), rows_here, width_in), jnp.bfloat16),
            pltpu.VMEM((rows_here, width_in), jnp.bfloat16),
            pair_sems(rep_total - 1),
            pair_sems(rep_total - 1),
        ],
        1,
        partial_value.reshape(rep_total, rows_here, width_in).astype(jnp.bfloat16),
        divisor,
        node_feats,
        self_weight,
        neigh_weight,
        out_grad,
    )
    group_spread = group_spread.reshape(group_blocks, TILE, width_in)
    grad_scale = 1.0 / math.sqrt(rows_here * dom_total * rep_total)
    picked_rows = group_spread[inbound_offset]
    products = jnp.einsum(
        "sij,sif->sjf", inbound_masks, picked_rows, preferred_element_type=jnp.float32
    )
    inner = math.gcd(dom_total, 4)
    outer = dom_total // inner
    plane = inner * rep_total
    strip = 2 * width_in // (dom_total * rep_total)
    both_grads, returned = call(
        functools.partial(finish, dom_total, rep_total, inner, grad_scale),
        (
            jax.ShapeDtypeStruct((plane, outer, strip, width_out), jnp.bfloat16),
            jax.ShapeDtypeStruct(products.shape, jnp.bfloat16),
        ),
        [
            pltpu.VMEM((max(plane - 1, 1), outer, strip, width_out), jnp.bfloat16),
            pltpu.VMEM((outer, strip, width_out), jnp.bfloat16),
            pltpu.VMEM((max(outer - 1, 1), strip, width_out), jnp.bfloat16),
            pltpu.VMEM((strip, width_out), jnp.bfloat16),
            pair_sems(plane - 1),
            pair_sems(outer - 1),
            pair_sems(outer - 1),
            pair_sems(plane - 1),
            pair_sems(dom_total - 1),
        ],
        2,
        both_terms.reshape(plane, outer, strip, width_out),
        products.astype(jnp.bfloat16),
    )
    both_grads = both_grads.reshape(2, width_in, width_out).astype(jnp.float32)
    returned = returned.astype(jnp.float32)
    transposed = jnp.einsum("db,djf->bjf", own_select, returned)
    feat_grad = (self_back + transposed.reshape(rows_here, width_in)).astype(jnp.bfloat16)
    return (hidden_out, feat_grad, both_grads[0], both_grads[1])


def solution(mesh):
    placed = (P(("dom", "rep"), None), P(), P(), P(), P(), P(), P(), P(("dom", "rep"), None))
    return jax.shard_map(
        shards,
        mesh=mesh,
        in_specs=placed,
        out_specs=(P(("dom", "rep"), None), P(("dom", "rep"), None), P(), P()),
        check_vma=False,
    )
```

```python
import functools
import math

import jax
import jax.numpy as jnp
from jax import lax
from jax.experimental import pallas as pl
from jax.experimental.pallas import tpu as pltpu
from jax.sharding import PartitionSpec as P

TILE = 128

MESH = pl.DeviceIdType.MESH
OVER_ROWS = (((0,), (0,)), ((), ()))
OVER_COLS = (((1,), (1,)), ((), ()))


def greet(devices):
    barrier = pltpu.get_barrier_semaphore()
    for device in devices:
        pl.semaphore_signal(barrier, inc=1, device_id=device, device_id_type=MESH)
    pl.semaphore_wait(barrier, len(devices))


def send(src, dst, sems, slot, device):
    copy = pltpu.make_async_remote_copy(
        src_ref=src,
        dst_ref=dst,
        send_sem=sems.at[0, slot],
        recv_sem=sems.at[1, slot],
        device_id=device,
        device_id_type=MESH,
    )
    copy.start()
    return copy


def dense(
    rep_total, partials, divisor, feats, w_self, w_neigh, cotangent,
    hidden, terms, back, gathered, landed, mine, sems_in, sems_out,
):
    dom, me = lax.axis_index("dom"), lax.axis_index("rep")
    peers = [lax.rem(me + k, rep_total) for k in range(1, rep_total)]
    greet([(dom, peer) for peer in peers])
    copies = [
        send(partials.at[peer], landed.at[k], sems_in, k, (dom, peer))
        for k, peer in enumerate(peers)
    ]
    x = feats[...]
    preact = jnp.dot(x, w_self[...], preferred_element_type=jnp.float32)
    summed = partials[me].astype(jnp.float32)
    for k, copy in enumerate(copies):
        copy.wait()
        summed = summed + landed[k].astype(jnp.float32)
    div = divisor[...]
    mean = (summed / div).astype(jnp.bfloat16)
    preact = preact + jnp.dot(mean, w_neigh[...], preferred_element_type=jnp.float32)
    logistic = jax.nn.sigmoid(preact)
    grad = (
        cotangent[...].astype(jnp.float32) * logistic * (1.0 + preact * (1.0 - logistic))
    ).astype(jnp.bfloat16)
    spread = lax.dot_general(grad, w_neigh[...], OVER_COLS, preferred_element_type=jnp.float32)
    mine[...] = (spread / div).astype(jnp.bfloat16)
    copies = [
        send(mine, gathered.at[me], sems_out, k, (dom, peer)) for k, peer in enumerate(peers)
    ]
    gathered[me] = mine[...]
    hidden[...] = (preact * logistic).astype(jnp.bfloat16)
    terms[0] = lax.dot_general(
        x, grad, OVER_ROWS, preferred_element_type=jnp.float32
    ).astype(jnp.bfloat16)
    terms[1] = lax.dot_general(
        mean, grad, OVER_ROWS, preferred_element_type=jnp.float32
    ).astype(jnp.bfloat16)
    back[...] = lax.dot_general(grad, w_self[...], OVER_COLS, preferred_element_type=jnp.float32)
    for copy in copies:
        copy.wait()


def finish(
    dom_total, rep_total, inner, scale, terms, grads,
    landed, share, strips, final, sems_a, sems_b, sems_c, sems_d,
):
    dom, rep = lax.axis_index("dom"), lax.axis_index("rep")
    outer = dom_total // inner
    plane = inner * rep_total
    layer, within = dom // inner, lax.rem(dom, inner)
    spot = within * rep_total + rep
    plane_peers = []
    for k in range(1, plane):
        other = lax.rem(spot + k, plane)
        plane_peers.append(
            (other, (layer * inner + other // rep_total, lax.rem(other, rep_total)))
        )
    layer_peers = []
    for k in range(1, outer):
        other = lax.rem(layer + k, outer)
        layer_peers.append((other, (other * inner + within, rep)))
    greet([device for _, device in plane_peers + layer_peers])
    first = [
        send(terms.at[other], landed.at[k], sems_a, k, device)
        for k, (other, device) in enumerate(plane_peers)
    ]
    total = terms[spot].astype(jnp.float32)
    for k, copy in enumerate(first):
        copy.wait()
        total = total + landed[k].astype(jnp.float32)
    share[...] = total.astype(jnp.bfloat16)
    second = [
        send(share.at[other], strips.at[k], sems_b, k, device)
        for k, (other, device) in enumerate(layer_peers)
    ]
    total = share[layer].astype(jnp.float32)
    for k, copy in enumerate(second):
        copy.wait()
        total = total + strips[k].astype(jnp.float32)
    final[...] = (total * scale).astype(jnp.bfloat16)
    third = [
        send(final, grads.at[spot, layer], sems_c, k, device)
        for k, (_, device) in enumerate(layer_peers)
    ]
    grads[spot, layer] = final[...]
    for copy in third:
        copy.wait()
    fourth = [
        send(grads.at[spot], grads.at[spot], sems_d, k, device)
        for k, (_, device) in enumerate(plane_peers)
    ]
    for copy in fourth:
        copy.wait()


def pair_sems(count):
    return pltpu.SemaphoreType.DMA((2, max(count, 1)))


def call(kernel, out_shapes, scratch, ident, *operands):
    return pl.pallas_call(
        kernel,
        out_shape=out_shapes,
        in_specs=[pl.BlockSpec(memory_space=pltpu.VMEM)] * len(operands),
        out_specs=jax.tree.map(lambda _: pl.BlockSpec(memory_space=pltpu.VMEM), out_shapes),
        scratch_shapes=scratch,
        compiler_params=pltpu.CompilerParams(collective_id=ident, has_side_effects=True),
        cost_estimate=pl.CostEstimate(
            flops=8_000_000_000, bytes_accessed=4_000_000, transcendentals=0
        ),
    )(*operands)


def edge_masks(row_ids, col_ids, limits, tile_size):
    left_ids = (row_ids % 4093)[:, :, None]
    right_ids = (col_ids % 4091)[:, None, :]
    hashed = (left_ids * right_ids + left_ids + 3 * right_ids) % 4099 % tile_size
    return (hashed < limits[:, None, None]).astype(jnp.bfloat16)


def shards(
    node_feats, node_ids, tile_row, tile_col, tile_count, self_weight, neigh_weight, out_grad
):
    dom_total = lax.axis_size("dom")
    rep_total = lax.axis_size("rep")
    dom_here = lax.axis_index("dom")
    rep_here = lax.axis_index("rep")
    rows_here, width_in = node_feats.shape
    blocks_here = rows_here // TILE
    group_blocks = blocks_here * rep_total
    id_blocks = node_ids.reshape(-1, TILE)
    group_first = dom_here * group_blocks
    own_first = group_first + rep_here * blocks_here
    inbound_rows = tile_row[dom_here, rep_here]
    inbound_present = inbound_rows >= 0
    inbound_block = jnp.where(inbound_present, inbound_rows, 0)
    inbound_cols = jnp.where(inbound_present, tile_col[dom_here, rep_here], 0)
    inbound_limits = jnp.where(inbound_present, tile_count[dom_here, rep_here], 0)
    inbound_masks = edge_masks(
        id_blocks[inbound_block], id_blocks[inbound_cols], inbound_limits, TILE
    )
    inbound_offset = jnp.where(inbound_present, inbound_block - group_first, 0)
    row_select = (
        (jnp.arange(group_blocks)[:, None] == inbound_offset[None, :]) & inbound_present[None, :]
    ).astype(jnp.float32)
    outbound_cols = tile_col[:, rep_here, dom_here]
    outbound_present = outbound_cols >= 0
    outbound_offset = jnp.where(outbound_present, outbound_cols - own_first, 0)
    own_select = (
        (outbound_offset[:, None] == jnp.arange(blocks_here)[None, :]) & outbound_present[:, None]
    ).astype(jnp.float32)
    feat_blocks = node_feats.reshape(blocks_here, TILE, width_in)
    outgoing = feat_blocks[outbound_offset]
    products = jnp.einsum(
        "sij,sjf->sif",
        inbound_masks,
        lax.all_to_all(outgoing, "dom", split_axis=0, concat_axis=0, tiled=True),
        preferred_element_type=jnp.float32,
    )
    partial_value = jnp.einsum("bs,sif->bif", row_select, products)
    group_rows = tile_row[dom_here].reshape(-1)
    group_limits = tile_count[dom_here].reshape(-1)
    owned_rows = group_rows[:, None] == own_first + jnp.arange(blocks_here)[None, :]
    degree = jnp.sum(jnp.where(owned_rows, group_limits[:, None], 0), axis=0).astype(jnp.float32)
    divisor = jnp.repeat(jnp.maximum(degree, 1.0), TILE)[:, None]
    width_out = self_weight.shape[1]
    hidden_out, both_terms, self_back, group_spread = call(
        functools.partial(dense, rep_total),
        (
            jax.ShapeDtypeStruct((rows_here, width_out), jnp.bfloat16),
            jax.ShapeDtypeStruct((2, width_in, width_out), jnp.bfloat16),
            jax.ShapeDtypeStruct((rows_here, width_in), jnp.float32),
            jax.ShapeDtypeStruct((rep_total, rows_here, width_in), jnp.bfloat16),
        ),
        [
            pltpu.VMEM((max(rep_total - 1, 1), rows_here, width_in), jnp.bfloat16),
            pltpu.VMEM((rows_here, width_in), jnp.bfloat16),
            pair_sems(rep_total - 1),
            pair_sems(rep_total - 1),
        ],
        1,
        partial_value.reshape(rep_total, rows_here, width_in).astype(jnp.bfloat16),
        divisor,
        node_feats,
        self_weight,
        neigh_weight,
        out_grad,
    )
    group_spread = group_spread.reshape(group_blocks, TILE, width_in)
    grad_scale = 1.0 / math.sqrt(rows_here * dom_total * rep_total)
    picked_rows = group_spread[inbound_offset]
    products = jnp.einsum(
        "sij,sif->sjf", inbound_masks, picked_rows, preferred_element_type=jnp.float32
    )
    inner = math.gcd(dom_total, 4)
    outer = dom_total // inner
    plane = inner * rep_total
    strip = 2 * width_in // (dom_total * rep_total)
    returned = lax.all_to_all(
        products.astype(jnp.bfloat16), "dom", split_axis=0, concat_axis=0, tiled=True
    )
    both_grads = call(
        functools.partial(finish, dom_total, rep_total, inner, grad_scale),
        jax.ShapeDtypeStruct((plane, outer, strip, width_out), jnp.bfloat16),
        [
            pltpu.VMEM((max(plane - 1, 1), outer, strip, width_out), jnp.bfloat16),
            pltpu.VMEM((outer, strip, width_out), jnp.bfloat16),
            pltpu.VMEM((max(outer - 1, 1), strip, width_out), jnp.bfloat16),
            pltpu.VMEM((strip, width_out), jnp.bfloat16),
            pair_sems(plane - 1),
            pair_sems(outer - 1),
            pair_sems(outer - 1),
            pair_sems(plane - 1),
        ],
        2,
        both_terms.reshape(plane, outer, strip, width_out),
    )
    both_grads = both_grads.reshape(2, width_in, width_out).astype(jnp.float32)
    returned = returned.astype(jnp.float32)
    transposed = jnp.einsum("db,djf->bjf", own_select, returned)
    feat_grad = (self_back + transposed.reshape(rows_here, width_in)).astype(jnp.bfloat16)
    return (hidden_out, feat_grad, both_grads[0], both_grads[1])


def solution(mesh):
    placed = (P(("dom", "rep"), None), P(), P(), P(), P(), P(), P(), P(("dom", "rep"), None))
    return jax.shard_map(
        shards,
        mesh=mesh,
        in_specs=placed,
        out_specs=(P(("dom", "rep"), None), P(("dom", "rep"), None), P(), P()),
        check_vma=False,
    )
```
